32 devices in a mesh: rep: 4 (over z), exp: 4 (over x, core), shard: 2 (over y).
Axes of the slice: x: 2, y: 2, z: 4, core: 2. Of those that a mesh axis runs over, the one named last changes fastest.
Arguments:
- tokens: bfloat16 [3584, 2048], P(('rep', 'exp', 'shard')), may hold values from -1.5 to 1.5
- routes: int32 [3584, 2], P(('rep', 'exp', 'shard')), may hold values from 0 to 3, all different within a row; in each aligned block of 112 rows (0 to 111, 112 to 223, ...) at most 63 rows name the same one
- gate_weight: bfloat16 [4, 2048, 7168], P('exp', None, 'shard'), may hold values from -0.125 to 0.125
- gate_cotangent: bfloat16 [4, 2016, 7168], P('exp', 'rep', 'shard'), may hold values from -0.75 to 0.75
Outputs:
- token_grad: bfloat16 [3584, 2048], P(('rep', 'exp', 'shard'))
- weight_grad: bfloat16 [4, 2048, 7168], P('exp', None, 'shard')
The draws below stay inside these ranges and needn't reach their ends.
Inputs may be any that keep to these rules, and one draw needn't show every extreme that they name: `routes`: the two entries of a row differ. The rows of one device name one expert at most 63 times, and some device names some expert exactly 63 times.
All inputs are finite; a program needn't handle non-finite values.
Results may differ from the reference program's by a relative error of at most 0.015.
Values may be sent and summed in bfloat16 or wider, within the bound.
A program may use at most 128 MiB of HBM per device.

```python
import math
import jax
import jax.numpy as jnp
import numpy as np
from jax import lax

DW = 2048
FFW = 7168
TOK_DEV = 112
EXPERTS = 4
TOKENS = 3584
SLOT_CAP = 63
SLOTS = 2016
N_REP = 4
N_EXP = 4
N_SHARD = 2


def shard_levels(rng, extent, pieces, least, high):
    gain = 1.0
    for dim, parts in pieces:
        steps = jax.random.uniform(jax.random.fold_in(jax.random.fold_in(rng, 6), dim), (parts,), jnp.float32, least / len(pieces), high / len(pieces))
        gain = gain * jnp.repeat(jnp.exp(steps), extent[dim] // parts).reshape((-1,) + (1,) * (len(extent) - 1 - dim))
    return gain


def routed_block(stream_key, own, number, rows, amount, top, most, lean):
    sequence = jax.random.permutation(stream_key, amount)
    packed, common = load_shares(amount, rows * top, most, lean, True), load_shares(amount, rows * top, most, lean, False)
    places = jnp.arange(amount)

    def named(tallies, rotation):
        used = int((tallies > 0).sum())
        fixed = max(1, used // 4)
        moved = fixed + (places - fixed + rotation * (used - fixed)) % max(1, amount - fixed)
        return jnp.zeros((amount,), jnp.int32).at[sequence[jnp.where(places < fixed, places, moved)]].set(jnp.asarray(tallies, jnp.int32))

    tallies = jnp.where(number % 4 == 0, named(packed, number // 4), named(common, number - number // 4 - 1))
    mixed = jax.random.permutation(jax.random.fold_in(own, 3), amount)
    source_of, taker = mixed[0:amount // 2 * 2:2], mixed[1:amount // 2 * 2:2]
    margin = jnp.minimum(tallies[source_of] - 1, most - tallies[taker]) // 2
    margin = jnp.where((source_of == sequence[0]) | (taker == sequence[0]) | (tallies[taker] == 0), 0, jnp.maximum(margin, 0))
    moved = jax.random.randint(jax.random.fold_in(own, 4), (amount // 2,), 0, 1 << 20) % (margin + 1)
    tallies = tallies.at[source_of].add(-moved).at[taker].add(moved)
    items = jnp.searchsorted(jnp.cumsum(tallies), jnp.arange(rows * top), side="right").astype(jnp.int32)
    listing = items.reshape(top, rows).T
    listing = listing[jax.random.permutation(jax.random.fold_in(own, 1), rows)]
    rotation = jax.random.randint(jax.random.fold_in(own, 2), (rows, 1), 0, top)
    return jnp.take_along_axis(listing, (jnp.arange(top)[None, :] + rotation) % top, axis=1)


def load_shares(number_of, total, limit, slope, full):
    portions = [(1 << 20) // math.isqrt(grade ** slope) + 1 for grade in range(1, number_of + 1)]
    largest = limit if full else min(limit, max(-(-total // number_of), total * portions[0] // sum(portions)))
    least = 1 if total - largest >= number_of - 1 else 0
    holding, surplus = [largest] + [least] * (number_of - 1), total - largest - least * (number_of - 1)
    while surplus > 0:
        free = [i for i in range(1, number_of) if holding[i] < largest] or [i for i in range(1, number_of) if holding[i] < limit]
        mass, left = sum([portions[i] for i in free]), surplus
        for i in free:
            more = min(limit - holding[i], max(1, left * portions[i] // mass), surplus)
            holding[i] = holding[i] + more
            surplus = surplus - more
    return np.array(holding)


def scatter_about(key, dims, spread, limit, split=(), kind=jnp.bfloat16):
    values = spread * jax.random.normal(key, dims, jnp.float32)
    if split:
        values = values * shard_levels(key, dims, split, -0.22, 0.18)
    return jnp.clip(values, -limit, limit).astype(kind)


def setup_inputs(seed: int = 0) -> dict:
    key_list = jax.random.split(jax.random.key(seed), 5)
    tokens = scatter_about(key_list[0], (TOKENS, DW), 0.25, 1.5, ((0, 32),))
    routes_keys = jax.random.split(jax.random.fold_in(key_list[1], 1), TOKENS // TOK_DEV)
    routes_turns = jax.random.permutation(jax.random.fold_in(key_list[1], 3), TOKENS // TOK_DEV)
    routes = jax.vmap(lambda own, number: routed_block(jax.random.fold_in(key_list[1], 2), own, number, TOK_DEV, EXPERTS, 2, SLOT_CAP, 2))(routes_keys, routes_turns).reshape((TOKENS, 2))
    gate_weight = scatter_about(key_list[2], (EXPERTS, DW, FFW), DW ** -0.5, 0.125, ((0, 4), (2, 2)))
    gate_cotangent = scatter_about(key_list[3], (EXPERTS, SLOTS, FFW), 0.125, 0.75, ((0, 4), (1, 4), (2, 2)))
    return {"tokens": tokens, "routes": routes, "gate_weight": gate_weight, "gate_cotangent": gate_cotangent}


def slot_matrix(route_rows, experts, slot_cap):
    expert_ids = jnp.arange(experts, dtype=jnp.int32)
    onehot = (route_rows[:, :, None] == expert_ids[None, None, :]).astype(jnp.int32)
    flattened = onehot.reshape(-1, experts)
    before = jnp.cumsum(flattened, axis=0) - flattened
    position = jnp.sum(before * flattened, axis=1)
    target = jnp.sum(flattened * expert_ids[None, :], axis=1) * slot_cap + position
    slot_ids = jnp.arange(experts * slot_cap, dtype=jnp.int32)
    matches = (target[None, :] == slot_ids[:, None]).astype(jnp.int32)
    return matches.reshape(experts * slot_cap, -1, 2).sum(axis=2)


def reference(tokens, routes, gate_weight, gate_cotangent):
    devices = N_REP * N_EXP * N_SHARD
    token_blocks = tokens.reshape(devices, TOK_DEV, DW).astype(jnp.float32)
    route_blocks = routes.reshape(devices, TOK_DEV, 2)

    def placing_of(route_rows):
        return slot_matrix(route_rows, EXPERTS, SLOT_CAP)

    placing = jax.vmap(placing_of)(route_blocks).astype(jnp.float32)
    outgoing = jnp.einsum("dst,dtw->dsw", placing, token_blocks).astype(jnp.bfloat16)
    grouped = outgoing.reshape(N_REP, N_EXP, N_SHARD, EXPERTS, SLOT_CAP, DW)
    grouped = grouped.transpose(3, 0, 1, 2, 4, 5).reshape(EXPERTS, SLOTS, DW)
    hidden_part = FFW // N_SHARD

    def per_expert(operands):
        gathered, cotangent, weights = operands
        weight_grad = jnp.dot(gathered.T, cotangent, preferred_element_type=jnp.float32).astype(jnp.bfloat16)
        summed = jnp.zeros((SLOTS, DW), jnp.float32)
        for shard_index in range(N_SHARD):
            lower = shard_index * hidden_part
            partial_value = jnp.dot(cotangent[:, lower:lower + hidden_part], weights[:, lower:lower + hidden_part].T,
                              preferred_element_type=jnp.float32).astype(jnp.bfloat16)
            partial_value = lax.optimization_barrier(partial_value)
            summed = summed + partial_value.astype(jnp.float32)
        return weight_grad, summed.astype(jnp.bfloat16)

    weight_grad, slot_grad = lax.map(per_expert, (grouped, gate_cotangent, gate_weight))
    returned = slot_grad.reshape(EXPERTS, N_REP, N_EXP, N_SHARD, SLOT_CAP, DW)
    returned = returned.transpose(1, 2, 3, 0, 4, 5).reshape(devices, EXPERTS * SLOT_CAP, DW)
    token_grad = jnp.einsum("dst,dsw->dtw", placing, returned.astype(jnp.float32)).astype(jnp.bfloat16)
    return token_grad.reshape(TOKENS, DW), weight_grad
```

```python
import jax
import jax.numpy as jnp
from jax import lax
from jax.experimental import pallas as pl
from jax.experimental.pallas import tpu as pltpu
from jax.sharding import PartitionSpec as P


def slot_matrix(route_rows, experts, slot_cap):
    expert_ids = jnp.arange(experts, dtype=jnp.int32)
    onehot = (route_rows[:, :, None] == expert_ids[None, None, :]).astype(jnp.int32)
    flattened = onehot.reshape(-1, experts)
    before = jnp.cumsum(flattened, axis=0) - flattened
    position = jnp.sum(before * flattened, axis=1)
    target = jnp.sum(flattened * expert_ids[None, :], axis=1) * slot_cap + position
    slot_ids = jnp.arange(experts * slot_cap, dtype=jnp.int32)
    matches = (target[None, :] == slot_ids[:, None]).astype(jnp.int32)
    return matches.reshape(experts * slot_cap, -1, 2).sum(axis=2)


def grad_kernel(*refs):
    rows_ref, cotangent_ref, out_ref = refs[0], refs[1], refs[-1]
    total = None
    for replica in range(rows_ref.shape[0]):
        term = jnp.dot(rows_ref[replica], cotangent_ref[replica], preferred_element_type=jnp.float32)
        total = term if total is None else total + term
    out_ref[0] = total.astype(out_ref.dtype)


def grad_columns(rows, cotangent, held, hidden, start, width):
    replicas, features, depth = rows.shape
    columns = cotangent.shape[2]
    tall = 512
    in_specs = [
        pl.BlockSpec((replicas, tall, depth), lambda j, i: (0, i, 0)),
        pl.BlockSpec((replicas, depth, width), lambda j, i: (0, 0, j)),
    ]
    operands = [rows, cotangent]
    aliases = {}
    if held is not None:
        in_specs.append(pl.BlockSpec(memory_space=pl.ANY))
        operands.append(held)
        aliases = {2: 0}
    first = start // width
    return pl.pallas_call(
        grad_kernel,
        grid=(columns // width, features // tall),
        in_specs=in_specs,
        out_specs=pl.BlockSpec((1, tall, width), lambda j, i: (0, i, j + first)),
        out_shape=jax.ShapeDtypeStruct((1, features, hidden), jnp.bfloat16),
        input_output_aliases=aliases,
        compiler_params=pltpu.CompilerParams(
            dimension_semantics=("arbitrary", "arbitrary"), vmem_limit_bytes=56 * 2**20
        ),
        cost_estimate=pl.CostEstimate(
            flops=2 * replicas * depth * features * columns,
            bytes_accessed=2 * (replicas * depth * (features + columns) + features * columns),
            transcendentals=0,
        ),
    )(*operands)


def body(tokens, routes, gate_weight, gate_cotangent):
    experts = lax.axis_size("exp")
    shards = lax.axis_size("shard")
    replicas = lax.axis_size("rep")
    features = tokens.shape[1]
    cotangent = gate_cotangent[0]
    rows, hidden = cotangent.shape
    slot_cap = rows // (experts * shards)
    weight = gate_weight[0]
    units = hidden // 128
    width = 128 * max(u for u in range(1, units + 1) if units % u == 0 and u <= max(1, units // 4))
    split = hidden - width

    all_tokens = lax.all_gather(tokens[None], "rep", axis=0, tiled=True)
    all_routes = lax.all_gather(routes[None], "rep", axis=0, tiled=True)
    first_part, all_tokens = lax.optimization_barrier((gate_cotangent[:, :, :split], all_tokens))
    first_all = lax.all_gather(first_part, "rep", axis=0, tiled=True)
    last_part, first_all = lax.optimization_barrier((gate_cotangent[:, :, split:], first_all))
    last_all = lax.all_gather(last_part, "rep", axis=0, tiled=True)

    placing_all = jax.vmap(lambda r: slot_matrix(r, experts, slot_cap))(all_routes).astype(jnp.bfloat16)
    outgoing = lax.dot_general(
        placing_all, all_tokens, (((2,), (1,)), ((0,), (0,))), preferred_element_type=jnp.float32
    ).astype(jnp.bfloat16)
    outgoing = outgoing.reshape(replicas, experts, slot_cap, features).swapaxes(0, 1)
    copies = jnp.broadcast_to(outgoing[:, None], (experts, shards, replicas, slot_cap, features))
    copies = copies.reshape(experts * shards, replicas, slot_cap, features)
    arrived = lax.all_to_all(copies, ("exp", "shard"), split_axis=0, concat_axis=0, tiled=True)
    gathered = arrived.swapaxes(0, 1).reshape(replicas, rows, features)
    lifted = gathered.swapaxes(1, 2)

    placing = slot_matrix(routes, experts, slot_cap).astype(jnp.bfloat16)
    blocks = cotangent.reshape(experts, shards, slot_cap, hidden)
    ordered = jnp.swapaxes(blocks, 0, 1).reshape(-1, hidden)
    summed = lax.psum_scatter(
        lax.dot_general(
            ordered, weight, (((1,), (1,)), ((), ())), preferred_element_type=jnp.float32
        ).astype(jnp.bfloat16),
        "shard",
        scatter_dimension=0,
        tiled=True,
    )
    slot_grad = summed.reshape(experts, slot_cap, features)
    returned = lax.all_to_all(slot_grad, "exp", split_axis=0, concat_axis=0, tiled=True)
    token_grad = jnp.dot(
        placing.T, returned.reshape(-1, features), preferred_element_type=jnp.float32
    ).astype(jnp.bfloat16)

    lifted, token_grad = lax.optimization_barrier((lifted, token_grad))
    weight_grad = grad_columns(lifted, first_all, None, hidden, 0, width)
    weight_grad = grad_columns(lifted, last_all, weight_grad, hidden, split, width)
    return (token_grad, weight_grad)


def solution(mesh):
    placed = (
        P(("rep", "exp", "shard"), None),
        P(("rep", "exp", "shard"), None),
        P("exp", None, "shard"),
        P("exp", "rep", "shard"),
    )
    return jax.shard_map(
        body,
        mesh=mesh,
        in_specs=placed,
        out_specs=(P(("rep", "exp", "shard"), None), P("exp", None, "shard")),
        check_vma=False,
    )
```

```python
import jax
import jax.numpy as jnp
from jax import lax
from jax.experimental import pallas as pl
from jax.experimental.pallas import tpu as pltpu
from jax.sharding import PartitionSpec as P


def slot_matrix(route_rows, experts, slot_cap):
    expert_ids = jnp.arange(experts, dtype=jnp.int32)
    onehot = (route_rows[:, :, None] == expert_ids[None, None, :]).astype(jnp.int32)
    flattened = onehot.reshape(-1, experts)
    before = jnp.cumsum(flattened, axis=0) - flattened
    position = jnp.sum(before * flattened, axis=1)
    target = jnp.sum(flattened * expert_ids[None, :], axis=1) * slot_cap + position
    slot_ids = jnp.arange(experts * slot_cap, dtype=jnp.int32)
    matches = (target[None, :] == slot_ids[:, None]).astype(jnp.int32)
    return matches.reshape(experts * slot_cap, -1, 2).sum(axis=2)


def grad_kernel(*refs):
    rows_ref, cotangent_ref, out_ref = refs[0], refs[1], refs[-1]
    total = None
    for replica in range(rows_ref.shape[0]):
        term = jnp.dot(rows_ref[replica], cotangent_ref[replica], preferred_element_type=jnp.float32)
        total = term if total is None else total + term
    out_ref[0] = total.astype(out_ref.dtype)


def grad_columns(rows, cotangent, held, hidden, start, width):
    replicas, features, depth = rows.shape
    columns = cotangent.shape[2]
    tall = 512
    in_specs = [
        pl.BlockSpec((replicas, tall, depth), lambda j, i: (0, i, 0)),
        pl.BlockSpec((replicas, depth, width), lambda j, i: (0, 0, j)),
    ]
    operands = [rows, cotangent]
    aliases = {}
    if held is not None:
        in_specs.append(pl.BlockSpec(memory_space=pl.ANY))
        operands.append(held)
        aliases = {2: 0}
    first = start // width
    return pl.pallas_call(
        grad_kernel,
        grid=(columns // width, features // tall),
        in_specs=in_specs,
        out_specs=pl.BlockSpec((1, tall, width), lambda j, i: (0, i, j + first)),
        out_shape=jax.ShapeDtypeStruct((1, features, hidden), jnp.bfloat16),
        input_output_aliases=aliases,
        compiler_params=pltpu.CompilerParams(
            dimension_semantics=("arbitrary", "arbitrary"), vmem_limit_bytes=56 * 2**20
        ),
        cost_estimate=pl.CostEstimate(
            flops=2 * replicas * depth * features * columns,
            bytes_accessed=2 * (replicas * depth * (features + columns) + features * columns),
            transcendentals=0,
        ),
    )(*operands)


def widest(columns, least):
    sizes = [least * u for u in range(1, columns // least + 1) if columns % (least * u) == 0]
    return max(c for c in sizes if c <= max(least, 1024))


def body(tokens, routes, gate_weight, gate_cotangent):
    experts = lax.axis_size("exp")
    shards = lax.axis_size("shard")
    replicas = lax.axis_size("rep")
    features = tokens.shape[1]
    cotangent = gate_cotangent[0]
    rows, hidden = cotangent.shape
    slot_cap = rows // (experts * shards)
    weight = gate_weight[0]
    units = hidden // 128
    width = 128 * max(u for u in range(1, units + 1) if units % u == 0 and u <= max(1, units // 7))
    split = hidden - width

    first_all = lax.all_gather(gate_cotangent[:, :, :split], "rep", axis=0, tiled=True)
    all_routes = lax.all_gather(routes[None], "rep", axis=0, tiled=True)
    half = tokens.shape[0] // 2
    upper = lax.all_gather(tokens[None, :half], "rep", axis=0, tiled=True)
    lower, upper = lax.optimization_barrier((tokens[None, half:], upper))
    lower = lax.all_gather(lower, "rep", axis=0, tiled=True)
    all_tokens = jnp.concatenate([upper, lower], axis=1)

    placing_all = jax.vmap(lambda r: slot_matrix(r, experts, slot_cap))(all_routes).astype(jnp.bfloat16)
    outgoing = lax.dot_general(
        placing_all, all_tokens, (((2,), (1,)), ((0,), (0,))), preferred_element_type=jnp.float32
    ).astype(jnp.bfloat16)
    outgoing = outgoing.reshape(replicas, experts, slot_cap, features).swapaxes(0, 1)
    copies = jnp.broadcast_to(outgoing[:, None], (experts, shards, replicas, slot_cap, features))
    copies = copies.reshape(experts * shards, replicas, slot_cap, features)
    copies, cotangent = lax.optimization_barrier((copies, cotangent))
    arrived = lax.all_to_all(copies, ("exp", "shard"), split_axis=0, concat_axis=0, tiled=True)

    placing = slot_matrix(routes, experts, slot_cap).astype(jnp.bfloat16)
    blocks = cotangent.reshape(experts, shards, slot_cap, hidden)
    ordered = jnp.swapaxes(blocks, 0, 1).reshape(-1, hidden)
    summed = lax.psum_scatter(
        lax.dot_general(
            ordered, weight, (((1,), (1,)), ((), ())), preferred_element_type=jnp.float32
        ).astype(jnp.bfloat16),
        "shard",
        scatter_dimension=0,
        tiled=True,
    )
    arrived, summed = lax.optimization_barrier((arrived, summed))
    gathered = arrived.swapaxes(0, 1).reshape(replicas, rows, features)
    lifted = gathered.swapaxes(1, 2)
    slot_grad = summed.reshape(experts, slot_cap, features)
    returned = lax.all_to_all(slot_grad, "exp", split_axis=0, concat_axis=0, tiled=True)
    token_grad = jnp.dot(
        placing.T, returned.reshape(-1, features), preferred_element_type=jnp.float32
    ).astype(jnp.bfloat16)

    last_part, first_all, lifted = lax.optimization_barrier(
        (gate_cotangent[:, :, split:], first_all, lifted)
    )
    last_all = lax.all_gather(last_part, "rep", axis=0, tiled=True)
    weight_grad = grad_columns(lifted, first_all, None, hidden, 0, widest(split, width))
    weight_grad = grad_columns(lifted, last_all, weight_grad, hidden, split, width)
    return (token_grad, weight_grad)


def solution(mesh):
    placed = (
        P(("rep", "exp", "shard"), None),
        P(("rep", "exp", "shard"), None),
        P("exp", None, "shard"),
        P("exp", "rep", "shard"),
    )
    return jax.shard_map(
        body,
        mesh=mesh,
        in_specs=placed,
        out_specs=(P(("rep", "exp", "shard"), None), P("exp", None, "shard")),
        check_vma=False,
    )
```
